32 devices in a mesh: groups: 2 (over x), ep: 16 (over z, y, core).
Axes of the slice: x: 2, y: 2, z: 4, core: 2. Of those that a mesh axis runs over, the one named last changes fastest.
Arguments:
- tokens: bfloat16 [4096, 3584], P(('groups', 'ep')), parts along dimension 0, may hold values from -6 to 6
- host: int32 [4096, 2], P(('groups', 'ep')), parts along dimension 0, may hold values from 0 to 7, all different within a row; in each aligned block of 128 rows (0 to 127, 128 to 255, ...) at most 40 rows name the same one
- copy: int32 [4096, 2], P(('groups', 'ep')), parts along dimension 0, may hold values from 0 to 1
- gate_prob: float32 [4096, 2], P(('groups', 'ep')), parts along dimension 0, may hold values from 0.1 to 1
- hot: int32 [8], replicated, may hold values from 0 to 7, each once
- w_gate: bfloat16 [16, 1792, 1024], P('ep'), may hold values from -0.09375 to 0.09375
- w_up: bfloat16 [16, 1792, 1024], P('ep'), may hold values from -0.09375 to 0.09375
- w_down: bfloat16 [16, 1024, 1792], P('ep'), may hold values from -0.1875 to 0.1875
- gate_scale: float32 [16, 14, 8], P('ep'), may hold values from 0.3 to 3
- up_scale: float32 [16, 14, 8], P('ep'), may hold values from 0.3 to 3
- down_scale: float32 [16, 8, 14], P('ep'), may hold values from 0.3 to 3
Outputs:
- mixed: bfloat16 [4096, 3584], P(('groups', 'ep')), parts along dimension 0
The draws below stay inside these ranges and needn't reach their ends.
There are 2 independent parts, one for each index of `groups`. The reference program is written for one: setup_inputs(seed, part) draws one part's arguments, and reference() takes and returns one part's arrays. A program takes and returns all parts, laid end to end along the dimension named above; an argument that names none is the same for every part. Nothing has to cross between parts.
Inputs may be any that keep to these rules, and one draw needn't show every extreme that they name: Each row names 2 different host groups; no group is named by more than 40 of the rows of one device. `hot`: A permutation of the 8 experts.
All inputs are finite; a program needn't handle non-finite values.
Results may differ from the reference program's by a relative error of at most 0.0087.
Values may be sent and summed in bfloat16 or wider, within the bound.
No kernel may reach another device: no remote copies, remote signals or barrier semaphores. Data moves between devices by JAX's collectives and lax.ppermute only.
A program may use at most 192 MiB of HBM per device.

```python
import math
import jax
import jax.numpy as jnp
import numpy as np
from jax import lax

D = 3584
HIDDEN_SIZE = 1024
BLOCK = 128
SPLIT = 2
TOP = 2
TOK_DEV = 128
EXPERTS = 8
CAP = 40
TOKENS = 2048
N_EP = 16


def touch_ends(array, rng, low, largest):
    shape = array.shape
    index_at = [jax.random.randint(jax.random.fold_in(rng, axis), (), 0, shape[axis]) for axis in range(len(shape))]
    array = array.at[tuple(index_at)].set(low)
    longest = shape.index(max(shape))
    index_at[longest] = (index_at[longest] + 1) % shape[longest]
    return array.at[tuple(index_at)].set(largest)


def steps_of(key, extent, cuts, smallest, largest):
    loudness, own = 1.0, jax.random.fold_in(key, 6)
    for position, parts in cuts:
        steps = jnp.exp(jax.random.uniform(jax.random.fold_in(own, position), (parts,), jnp.float32, smallest / len(cuts), largest / len(cuts)))
        loudness = loudness * jnp.repeat(steps, extent[position] // parts).reshape([-1 if axis == position else 1 for axis in range(len(extent))])
    return loudness


def shared_out(rng, own, number, rows, amount, top, limit, slope):
    sequence = jax.random.permutation(rng, amount)
    packed, common = load_shares(amount, rows * top, limit, slope, True), load_shares(amount, rows * top, limit, slope, False)
    places = jnp.arange(amount)

    def named(tallies, rotation):
        used = int((tallies > 0).sum())
        fixed = max(1, used // 4)
        shifted = fixed + (places - fixed + rotation * (used - fixed)) % max(1, amount - fixed)
        return jnp.zeros((amount,), jnp.int32).at[sequence[jnp.where(places < fixed, places, shifted)]].set(jnp.asarray(tallies, jnp.int32))

    tallies = jnp.where(number % 4 == 0, named(packed, number // 4), named(common, number - number // 4 - 1))
    mixed = jax.random.permutation(jax.random.fold_in(own, 3), amount)
    source_of, sink = mixed[0:amount // 2 * 2:2], mixed[1:amount // 2 * 2:2]
    slack = jnp.minimum(tallies[source_of] - 1, limit - tallies[sink]) // 2
    slack = jnp.where((source_of == sequence[0]) | (sink == sequence[0]) | (tallies[sink] == 0), 0, jnp.maximum(slack, 0))
    shifted = jax.random.randint(jax.random.fold_in(own, 4), (amount // 2,), 0, 1 << 20) % (slack + 1)
    tallies = tallies.at[source_of].add(-shifted).at[sink].add(shifted)
    items = jnp.searchsorted(jnp.cumsum(tallies), jnp.arange(rows * top), side="right").astype(jnp.int32)
    table = items.reshape(top, rows).T
    table = table[jax.random.permutation(jax.random.fold_in(own, 1), rows)]
    rotation = jax.random.randint(jax.random.fold_in(own, 2), (rows, 1), 0, top)
    return jnp.take_along_axis(table, (jnp.arange(top)[None, :] + rotation) % top, axis=1)


def load_shares(number_of, total, limit, skew, full):
    weights = [(1 << 20) // math.isqrt(standing ** skew) + 1 for standing in range(1, number_of + 1)]
    largest = limit if full else min(limit, max(-(-total // number_of), total * weights[0] // sum(weights)))
    least = 1 if total - largest >= number_of - 1 else 0
    counts, spare = [largest] + [least] * (number_of - 1), total - largest - least * (number_of - 1)
    while spare > 0:
        free = [i for i in range(1, number_of) if counts[i] < largest] or [i for i in range(1, number_of) if counts[i] < limit]
        pool, left = sum([weights[i] for i in free]), spare
        for i in free:
            addition = min(limit - counts[i], max(1, left * weights[i] // pool), spare)
            counts[i] = counts[i] + addition
            spare = spare - addition
    return np.array(counts)


def centred(own_key, dims, width, limit, pieces=(), kind=jnp.bfloat16):
    array = jax.random.normal(own_key, dims, jnp.float32) * width
    if len(pieces) > 0:
        array = steps_of(own_key, dims, pieces, -0.22, 0.18) * array
    return jnp.clip(array, min=-limit, max=limit).astype(kind)


def setup_inputs(seed: int = 0, part: int = 0) -> dict:
    splits = jax.random.split(jax.random.key(seed), 12)
    part_keys = jax.random.split(jax.random.fold_in(splits[11], part), 12)
    tokens = centred(part_keys[0], (TOKENS, D), 1.0, 6.0, ((0, 16),))
    host_keys = jax.random.split(jax.random.fold_in(part_keys[1], 1), TOKENS // TOK_DEV)
    host_turns = jax.random.permutation(jax.random.fold_in(part_keys[1], 3), TOKENS // TOK_DEV)
    host = jax.vmap(lambda own, number: shared_out(jax.random.fold_in(part_keys[1], 2), own, number, TOK_DEV, EXPERTS, TOP, CAP, 2))(host_keys, host_turns).reshape((TOKENS, TOP))
    copy = touch_ends(jax.random.randint(part_keys[2], (TOKENS, TOP), 0, 2), jax.random.fold_in(part_keys[2], 1), 0, 1).astype(jnp.int32)
    gate_prob = jnp.clip(jnp.exp(math.log(1.0) - 2.3025851 * jax.random.uniform(part_keys[3], (TOKENS, TOP), jnp.float32) ** steps_of(part_keys[3], (TOKENS, TOP), ((0, 16),), -0.2, 0.2)), 0.1, 1.0)
    hot = jax.random.permutation(splits[4], EXPERTS).astype(jnp.int32)
    w_gate = centred(splits[5], (EXPERTS * SPLIT, D // SPLIT, HIDDEN_SIZE), D ** -0.5, 0.09375, ((0, 16),))
    w_up = centred(splits[6], (EXPERTS * SPLIT, D // SPLIT, HIDDEN_SIZE), D ** -0.5, 0.09375, ((0, 16),))
    w_down = centred(splits[7], (EXPERTS * SPLIT, HIDDEN_SIZE, D // SPLIT), HIDDEN_SIZE ** -0.5, 0.1875, ((0, 16),))
    gate_scale = jnp.clip(jnp.exp(math.log(3.0) - 2.3025851 * jax.random.uniform(splits[8], (EXPERTS * SPLIT, D // SPLIT // BLOCK, HIDDEN_SIZE // BLOCK), jnp.float32) ** steps_of(splits[8], (EXPERTS * SPLIT, D // SPLIT // BLOCK, HIDDEN_SIZE // BLOCK), ((0, 16),), -0.2, 0.2)), 0.3, 3.0)
    up_scale = jnp.clip(jnp.exp(math.log(3.0) - 2.3025851 * jax.random.uniform(splits[9], (EXPERTS * SPLIT, D // SPLIT // BLOCK, HIDDEN_SIZE // BLOCK), jnp.float32) ** steps_of(splits[9], (EXPERTS * SPLIT, D // SPLIT // BLOCK, HIDDEN_SIZE // BLOCK), ((0, 16),), -0.2, 0.2)), 0.3, 3.0)
    down_scale = jnp.clip(jnp.exp(math.log(3.0) - 2.3025851 * jax.random.uniform(splits[10], (EXPERTS * SPLIT, HIDDEN_SIZE // BLOCK, D // SPLIT // BLOCK), jnp.float32) ** steps_of(splits[10], (EXPERTS * SPLIT, HIDDEN_SIZE // BLOCK, D // SPLIT // BLOCK), ((0, 16),), -0.2, 0.2)), 0.3, 3.0)
    return {"tokens": tokens, "host": host, "copy": copy, "gate_prob": gate_prob, "hot": hot, "w_gate": w_gate, "w_up": w_up, "w_down": w_down, "gate_scale": gate_scale, "up_scale": up_scale, "down_scale": down_scale}


def dequant(weight, scales):
    rows_in, cols_in = weight.shape
    row_blocks, col_blocks = scales.shape
    expanded = jnp.repeat(scales, cols_in // col_blocks, axis=1)
    blocks = weight.reshape(row_blocks, rows_in // row_blocks, cols_in).astype(jnp.float32) * expanded[:, None, :]
    return blocks.reshape(rows_in, cols_in).astype(jnp.bfloat16)


def widen(value):
    return lax.optimization_barrier(value.astype(jnp.bfloat16)).astype(jnp.float32)


def reference(tokens, host, copy, gate_prob, hot, w_gate, w_up, w_down, gate_scale, up_scale, down_scale):
    pair_count = TOKENS * TOP
    host_f = host.reshape(pair_count)
    copy_f = copy.reshape(pair_count)
    expert_f = jnp.where(copy_f == 0, host_f, hot[host_f]).astype(jnp.int32)
    weight_f = gate_prob.reshape(pair_count)
    limit_rows = 2 * N_EP * CAP
    half_width = D // SPLIT

    def one_expert(expert, running):
        expert = expert.astype(jnp.int32)
        matches = expert_f == expert
        live_count = jnp.sum(matches.astype(jnp.int32))
        picks = jnp.nonzero(matches, size=limit_rows, fill_value=0)[0].astype(jnp.int32)
        is_valid = (jnp.arange(limit_rows, dtype=jnp.int32) < live_count).astype(jnp.float32)
        chosen = tokens[picks // TOP]
        gate_sum = jnp.zeros((limit_rows, HIDDEN_SIZE), jnp.float32)
        up_sum = jnp.zeros((limit_rows, HIDDEN_SIZE), jnp.float32)
        for part_index in range(SPLIT):
            block_id = expert * SPLIT + part_index
            features = chosen[:, part_index * half_width:(part_index + 1) * half_width]
            gate_mat = dequant(lax.dynamic_index_in_dim(w_gate, block_id, 0, keepdims=False), lax.dynamic_index_in_dim(gate_scale, block_id, 0, keepdims=False))
            up_mat = dequant(lax.dynamic_index_in_dim(w_up, block_id, 0, keepdims=False), lax.dynamic_index_in_dim(up_scale, block_id, 0, keepdims=False))
            gate_sum = gate_sum + widen(jnp.dot(features, gate_mat, preferred_element_type=jnp.float32))
            up_sum = up_sum + widen(jnp.dot(features, up_mat, preferred_element_type=jnp.float32))
        hidden = (jax.nn.silu(gate_sum) * up_sum).astype(jnp.bfloat16)
        halves = []
        for part_index in range(SPLIT):
            block_id = expert * SPLIT + part_index
            down_mat = dequant(lax.dynamic_index_in_dim(w_down, block_id, 0, keepdims=False), lax.dynamic_index_in_dim(down_scale, block_id, 0, keepdims=False))
            halves.append(widen(jnp.dot(hidden, down_mat, preferred_element_type=jnp.float32)))
        expert_out = jnp.concatenate(halves, axis=1)
        contrib = expert_out * (weight_f[picks] * is_valid)[:, None]
        return running.at[picks // TOP].add(contrib)

    running = lax.fori_loop(0, EXPERTS, one_expert, jnp.zeros((TOKENS, D), jnp.float32))
    return running.astype(jnp.bfloat16)
```

```python
import functools

import jax
import jax.numpy as jnp
from jax import lax
from jax.experimental import pallas as pl
from jax.experimental.pallas import tpu as pltpu
from jax.sharding import PartitionSpec as P

SPLIT = 2
INNER = 2
LANES = 128

VMEM = pl.BlockSpec(memory_space=pltpu.VMEM)
SMEM = pl.BlockSpec(memory_space=pltpu.SMEM)


def f32(value):
    return value.astype(jnp.float32)


def bf16(value):
    return value.astype(jnp.bfloat16)


def dot(left, right):
    return jnp.dot(left, right, preferred_element_type=jnp.float32)


def pack_kernel(lane_ref, hot_ref, tok_ref, host_ref, copy_ref, prob_ref, out_ref):
    rows, width = tok_ref.shape
    half = width // SPLIT
    side = lane_ref[0]
    for part in range(SPLIT):
        start = pl.multiple_of((side ^ part) * half, LANES)
        out_ref[:, part * half : (part + 1) * half] = tok_ref[:, pl.ds(start, half)]
    column = lax.broadcasted_iota(jnp.int32, (rows, LANES), 1)
    meta = jnp.zeros((rows, LANES), jnp.float32)
    top = host_ref.shape[1]
    for choice in range(top):
        host = host_ref[:, choice : choice + 1]
        moved = jnp.zeros_like(host)
        for key in range(hot_ref.shape[0]):
            moved = jnp.where(host == key, hot_ref[key], moved)
        expert = jnp.where(copy_ref[:, choice : choice + 1] == 0, host, moved)
        prob = prob_ref[:, choice : choice + 1]
        high = f32(bf16(prob))
        middle = f32(bf16(prob - high))
        low = prob - high - middle
        base = 4 * choice
        meta = jnp.where(column == base, f32(expert + 1), meta)
        meta = jnp.where(column == base + 1, high, meta)
        meta = jnp.where(column == base + 2, middle, meta)
        meta = jnp.where(column == base + 3, low, meta)
    out_ref[:, width:] = bf16(meta)


def slots_of(meta, expert, top):
    rows = meta.shape[0]
    match = meta[:, 0:1] == expert
    for choice in range(1, top):
        match = match | (meta[:, 4 * choice : 4 * choice + 1] == expert)
    wide = jnp.broadcast_to(jnp.where(match, 1.0, 0.0), (rows, LANES))
    before = lax.broadcasted_iota(jnp.int32, (rows, rows), 1) < lax.broadcasted_iota(
        jnp.int32, (rows, rows), 0
    )
    position = dot(bf16(jnp.where(before, 1.0, 0.0)), bf16(wide))
    lane = f32(lax.broadcasted_iota(jnp.int32, (rows, LANES), 1))
    return jnp.where((position == lane) & (wide > 0.0), 1.0, 0.0)


def select_kernel(top, sources, slots, ids_ref, *refs):
    chunk = refs[0][...]
    for other in range(1, sources):
        chunk = chunk + refs[other][...]
    own_ref, next_ref, hot_ref = refs[sources:]
    meta = f32(chunk[:, chunk.shape[1] - LANES :])
    for place, out_ref in enumerate((own_ref, next_ref)):
        onehot = slots_of(meta, f32(ids_ref[place] + 1), top)
        hot_ref[:, place * LANES : (place + 1) * LANES] = bf16(onehot)
        out_ref[...] = bf16(dot(bf16(onehot.T[:slots]), chunk))


def expert_kernel(top, groups, ids_ref, *refs):
    rows_refs = refs[:groups]
    gate_a, gate_b, up_a, up_b, down_a, down_b = refs[groups : groups + 6]
    out_refs = refs[groups + 6 : 2 * groups + 6]
    x_ref, total = refs[2 * groups + 6 :]
    step = pl.program_id(0)
    half = gate_a.shape[0]
    width = SPLIT * half
    slots = rows_refs[0].shape[0]

    @pl.when(step == 0)
    def _():
        for group in range(groups):
            x_ref[group * slots : (group + 1) * slots, :] = rows_refs[group][...]
        total[...] = jnp.zeros_like(total)

    left, right = x_ref[:, :half], x_ref[:, half:width]
    gate = dot(left, gate_a[...]) + dot(right, gate_b[...])
    up = dot(left, up_a[...]) + dot(right, up_b[...])
    hidden = bf16(gate / (1.0 + jnp.exp(-gate)) * up)
    total[:, :half] += dot(hidden, down_a[...])
    total[:, half:] += dot(hidden, down_b[...])

    @pl.when(step == pl.num_programs(0) - 1)
    def _():
        meta = f32(x_ref[:, width:])
        mine = f32(ids_ref[0] + 1)
        weight = jnp.zeros((meta.shape[0], 1), jnp.float32)
        for choice in range(top):
            base = 4 * choice
            prob = meta[:, base + 1 : base + 2] + meta[:, base + 2 : base + 3]
            prob = prob + meta[:, base + 3 : base + 4]
            weight = weight + jnp.where(meta[:, base : base + 1] == mine, prob, 0.0)
        for group in range(groups):
            span = slice(group * slots, (group + 1) * slots)
            out_refs[group][...] = bf16(total[span, :] * weight[span])


def spread_kernel(slots, extras, final, ids_ref, hot_ref, own_ref, back_ref, *refs):
    out_ref = refs[extras]
    width = own_ref.shape[1]
    half = width // SPLIT
    for part in range(SPLIT):
        span = slice(part * half, (part + 1) * half)
        value = dot(hot_ref[:, :slots], own_ref[:, span])
        value = value + dot(hot_ref[:, LANES : LANES + slots], back_ref[:, span])
        for extra in range(extras):
            value = value + f32(refs[extra][:, span])
        if final:
            start = pl.multiple_of((ids_ref[2] ^ part) * half, LANES)
            out_ref[:, pl.ds(start, half)] = bf16(value)
        else:
            out_ref[:, span] = bf16(value)


def scale_kernel(row_blocks, block, scale_ref, in_ref, out_ref):
    step = pl.program_id(0)
    for row in range(row_blocks):
        rows = slice(row * block, (row + 1) * block)
        for col in range(scale_ref.shape[1]):
            cols = slice(col * block, (col + 1) * block)
            factor = scale_ref[step * row_blocks + row, col]
            out_ref[rows, cols] = bf16(f32(in_ref[rows, cols]) * factor)


def shape(*dims):
    return jax.ShapeDtypeStruct(dims, jnp.bfloat16)


def cost(flops, moved):
    return pl.CostEstimate(flops=flops, bytes_accessed=moved, transcendentals=0)


def dequant(weight, scales):
    rows, cols = weight.shape
    block = rows // scales.shape[0]
    row_blocks = 2 if scales.shape[0] % 2 == 0 else 1
    tall = block * row_blocks
    return pl.pallas_call(
        functools.partial(scale_kernel, row_blocks, block),
        grid=(rows // tall,),
        in_specs=[SMEM, pl.BlockSpec((tall, cols), lambda i: (i, 0))],
        out_specs=pl.BlockSpec((tall, cols), lambda i: (i, 0)),
        out_shape=shape(rows, cols),
        cost_estimate=cost(rows * cols * 400, rows * cols * 4),
        name="dequant",
    )(scales, weight)


def pack(ids, hot, tokens, host, copy, prob):
    rows, width = tokens.shape
    return pl.pallas_call(
        pack_kernel,
        in_specs=[SMEM, SMEM, VMEM, VMEM, VMEM, VMEM],
        out_specs=VMEM,
        out_shape=shape(rows, width + LANES),
        name="pack",
    )(ids[2:3], hot, tokens, host, copy, prob)


def select(ids, chunks, slots, top):
    rows, wide = chunks[0].shape
    return pl.pallas_call(
        functools.partial(select_kernel, top, len(chunks), slots),
        in_specs=[SMEM] + [VMEM] * len(chunks),
        out_specs=[VMEM] * 3,
        out_shape=[shape(slots, wide), shape(slots, wide), shape(rows, 2 * LANES)],
        cost_estimate=cost(1500000000, rows * wide * 6),
        name="select",
    )(ids, *chunks)


def run_expert(ids, row_groups, weights, top):
    slots, wide = row_groups[0].shape
    groups = len(row_groups)
    half, hidden = weights[0].shape
    width = half * SPLIT
    piece = 2 * LANES if hidden % (2 * LANES) == 0 else LANES
    tall = pl.BlockSpec((half, piece), lambda i: (0, i))
    flat = pl.BlockSpec((piece, half), lambda i: (i, 0))
    whole = pl.BlockSpec((slots, wide), lambda i: (0, 0))
    result = pl.BlockSpec((slots, width), lambda i: (0, 0))
    return pl.pallas_call(
        functools.partial(expert_kernel, top, groups),
        grid=(hidden // piece,),
        in_specs=[SMEM] + [whole] * groups + [tall] * 4 + [flat] * 2,
        out_specs=[result] * groups,
        out_shape=[shape(slots, width)] * groups,
        scratch_shapes=[
            pltpu.VMEM((groups * slots, wide), jnp.bfloat16),
            pltpu.VMEM((groups * slots, width), jnp.float32),
        ],
        cost_estimate=cost(groups * slots * width * hidden * 6, width * hidden * 6),
        name="expert",
    )(ids, *row_groups, *weights)


def spread(ids, onehot, own, back, extras, slots, final=False):
    rows, width = onehot.shape[0], own.shape[1]
    return pl.pallas_call(
        functools.partial(spread_kernel, slots, len(extras), final),
        in_specs=[SMEM] + [VMEM] * (3 + len(extras)),
        out_specs=VMEM,
        out_shape=shape(rows, width),
        cost_estimate=cost(1500000000, rows * width * 6),
        name="spread",
    )(ids, onehot, own, back, *extras)


def line_plan(tokens, host, copy, gate_prob, hot, weights_in, slots):
    devices = lax.axis_size("ep")
    experts = devices // SPLIT
    planes = experts // INNER
    stride = INNER * SPLIT
    top = host.shape[1]
    me = lax.axis_index("ep")
    expert = me // SPLIT
    ids = jnp.stack([expert, expert ^ 1, me % SPLIT]).astype(jnp.int32)

    def along(value, hop, froms):
        pairs = [
            (plane * stride + rest, (plane + hop) * stride + rest)
            for plane in froms
            for rest in range(stride)
        ]
        return lax.ppermute(value, "ep", pairs)

    def across(value, froms):
        pairs = [
            (plane * stride + rest, plane * stride + (rest ^ SPLIT))
            for plane in froms
            for rest in range(stride)
        ]
        return lax.ppermute(value, "ep", pairs)

    def beside(value):
        return lax.ppermute(value, "ep", [(s, s ^ 1) for s in range(devices)])

    every = list(range(planes))
    mine = pack(ids, hot, tokens, host, copy, gate_prob)
    up_of = lambda distance: [p for p in every if p + distance < planes]
    down_of = lambda distance: [p for p in every if p - distance >= 0]

    ups, downs = {}, {}
    for distance in range(1, planes):
        if distance == 2:
            ups[2] = along(ups[1], 1, [p + 1 for p in up_of(2)])
            downs[2] = along(downs[1], -1, [p - 1 for p in down_of(2)])
        else:
            ups[distance] = along(mine, distance, up_of(distance))
            downs[distance] = along(mine, -distance, down_of(distance))

    own_weights = [dequant(w, s) for w, s in weights_in]
    weights = []
    for held in own_weights:
        weights += [held, beside(held)]

    def prepare(chunks, valid):
        own, other, onehot = select(ids, chunks, slots, top)
        return own, across(other, valid), onehot

    def finish(outs, valid):
        return outs[0], across(outs[1], valid)

    def handle(members):
        ready = [prepare(chunks, valid) for chunks, valid in members]
        row_groups = [rows for own, other, _ in ready for rows in (own, other)]
        outs = run_expert(ids, row_groups, weights, top)
        result = []
        for at, ((_, valid), (_, _, onehot)) in enumerate(zip(members, ready)):
            own, back = finish(outs[2 * at : 2 * at + 2], valid)
            result.append((onehot, own, back))
        return result

    def dense(entry, extras=(), final=False):
        return spread(ids, *entry, extras, slots, final)

    arrivals = []
    (here,) = handle([([mine], every)])
    for distance in range(3, planes):
        members = [
            ([ups[distance]], [p + distance for p in up_of(distance)]),
            ([downs[distance]], [p - distance for p in down_of(distance)]),
        ]
        if 2 * distance >= planes:
            members = [(members[0][0] + members[1][0], members[0][1] + members[1][1])]
        entries = handle(members)
        if len(entries) == 1:
            back = dense(entries[0])
            arrivals.append(along(back, distance, [p - distance for p in down_of(distance)]))
            arrivals.append(along(back, -distance, [p + distance for p in up_of(distance)]))
        else:
            arrivals.append(along(dense(entries[0]), -distance, members[0][1]))
            arrivals.append(along(dense(entries[1]), distance, members[1][1]))
    if planes > 1:
        from_below, from_above = handle(
            [([ups[1]], [p + 1 for p in up_of(1)]), ([downs[1]], [p - 1 for p in down_of(1)])]
        )
        extra_below, extra_above = (), ()
        if planes > 2:
            valid_up = [p + 2 for p in up_of(2)]
            valid_down = [p - 2 for p in down_of(2)]
            if planes <= 4:
                (both,) = handle([([ups[2], downs[2]], valid_up + valid_down)])
                both = dense(both)
                two_below, two_above = both, both
            else:
                pair = handle([([ups[2]], valid_up), ([downs[2]], valid_down)])
                two_below, two_above = dense(pair[0]), dense(pair[1])
            extra_below = (along(two_below, -1, valid_up),)
            extra_above = (along(two_above, 1, valid_down),)
        arrivals.append(along(dense(from_below, extra_below), -1, [p + 1 for p in up_of(1)]))
        arrivals.append(along(dense(from_above, extra_above), 1, [p - 1 for p in down_of(1)]))
    return dense(here, tuple(arrivals), True)


def lookup(table_in, keys):
    positions = jnp.arange(table_in.shape[0], dtype=jnp.int32)
    return jnp.sum(jnp.where(keys[:, None] == positions[None, :], table_in[None, :], 0), axis=1)


def direct_plan(tokens, host, copy, gate_prob, hot, weights_in, zone_rows):
    devices = lax.axis_size("ep")
    experts = devices // SPLIT
    tok_rows, width = tokens.shape
    top_count = host.shape[1]
    half_width = width // SPLIT
    pair_count = tok_rows * top_count
    host_f = host.reshape(pair_count)
    copy_f = copy.reshape(pair_count)
    onehot = (host_f[:, None] == jnp.arange(experts, dtype=jnp.int32)[None, :]).astype(jnp.int32)
    slot_f = jnp.sum((jnp.cumsum(onehot, axis=0) - 1) * onehot, axis=1)
    expert_f = jnp.where(copy_f == 0, host_f, lookup(hot, host_f))
    place_f = copy_f * (zone_rows // 2) + slot_f
    tok_split = tokens.reshape(tok_rows, SPLIT, half_width)
    own_gate, own_up, own_down = [dequant(w, s) for w, s in weights_in]
    slots_all = experts * zone_rows
    slot_table = (
        jnp.zeros((slots_all,), jnp.int32)
        .at[expert_f * zone_rows + place_f]
        .set(jnp.arange(pair_count, dtype=jnp.int32) + 1)
    )
    slot_table = slot_table.reshape(experts, zone_rows)
    filled = slot_table > 0
    row_of = jnp.maximum(slot_table - 1, 0) // top_count
    picked = tok_split[row_of[:, None, :], jnp.arange(SPLIT, dtype=jnp.int32)[None, :, None]]
    picked = jnp.where(filled[:, None, :, None], picked, jnp.zeros_like(picked))
    outgoing_rows = picked.reshape(devices, zone_rows, half_width)
    received = lax.all_to_all(outgoing_rows, "ep", split_axis=0, concat_axis=0, tiled=True)
    gate_part = bf16(dot(received, own_gate))
    up_part = bf16(dot(received, own_up))
    pairs = [(source, source ^ 1) for source in range(devices)]
    partner_gate, partner_up = lax.ppermute((gate_part, up_part), "ep", pairs)
    gate_sum = f32(gate_part) + f32(partner_gate)
    up_sum = f32(up_part) + f32(partner_up)
    hidden = bf16(jax.nn.silu(gate_sum) * up_sum)
    results = bf16(dot(hidden, own_down))
    returned = lax.all_to_all(results, "ep", split_axis=0, concat_axis=0, tiled=True)
    back_four = returned.reshape(experts, SPLIT, zone_rows, half_width)
    values = back_four[
        expert_f[:, None], jnp.arange(SPLIT, dtype=jnp.int32)[None, :], place_f[:, None]
    ]
    values = f32(values.reshape(tok_rows, top_count, width))
    return bf16(jnp.sum(values * gate_prob[:, :, None], axis=1))


def per_device(
    tokens, host, copy, gate_prob, hot, w_gate, w_up, w_down, gate_scale, up_scale, down_scale
):
    experts = lax.axis_size("ep") // SPLIT
    tok_rows, top_count = host.shape
    zone_rows = 2 * (tok_rows * top_count * 5 // (4 * experts))
    weights_in = [
        (w_gate[0], gate_scale[0]),
        (w_up[0], up_scale[0]),
        (w_down[0], down_scale[0]),
    ]
    slots = min(zone_rows, tok_rows)
    if tok_rows <= 2 * zone_rows and slots % 16 == 0 and experts % INNER == 0:
        return line_plan(tokens, host, copy, gate_prob, hot, weights_in, slots)
    return direct_plan(tokens, host, copy, gate_prob, hot, weights_in, zone_rows)


def solution(mesh):
    return jax.shard_map(
        per_device,
        mesh=mesh,
        in_specs=(
            P(("groups", "ep"), None),
            P(("groups", "ep"), None),
            P(("groups", "ep"), None),
            P(("groups", "ep"), None),
            P(),
            P("ep", None, None),
            P("ep", None, None),
            P("ep", None, None),
            P("ep", None, None),
            P("ep", None, None),
            P("ep", None, None),
        ),
        out_specs=P(("groups", "ep"), None),
        check_vma=False,
    )
```
